256 devices in a mesh: grp: 4 (over y), row: 64 (over x, z, core).
Axes of the slice: x: 4, y: 4, z: 8, core: 2. Of those that a mesh axis runs over, the one named last changes fastest.
Arguments:
- embeds: bfloat16 [32768, 384], P(('grp', 'row')), may hold values from -6 to 6
- w_hidden: bfloat16 [384, 384], replicated, may hold values from -0.3125 to 0.3125
- b_hidden: float32 [384], replicated, may hold values from -3 to 3
- w_out: bfloat16 [384, 128], replicated, may hold values from -0.3125 to 0.3125
- probes: int32 [16, 32768], P(None, ('grp', 'row')), may hold values from 0 to 1
Outputs:
- solves: float32 [16, 32768], P(None, ('grp', 'row'))
- logdet_rate: float32 [16], replicated
- scale_grad: float32 [16], replicated
The draws below stay inside these ranges and needn't reach their ends.
All inputs are finite; a program needn't handle non-finite values.
Results may differ from the reference program's by a relative error of at most 0.0085.
Values may be sent and summed in bfloat16 or wider, within the bound.
A program may use at most 128 MiB of HBM per device.

```python
import math
import jax
import jax.numpy as jnp
from jax import lax

EMB = 384
FEAT = 128
PROBES = 16
ITERS = 8
SWEEPS = 6
ROWS = 32768


def draw_embeds(key, part):
    key_perm, key_center, key_jitter, key_scale = jax.random.split(jax.random.fold_in(key, 11), 4)
    copies = 8
    shuffled = jax.random.permutation(key_perm, ROWS)
    members = shuffled // copies
    group_count = ROWS // copies
    centers = jax.random.normal(key_center, (group_count, EMB), jnp.float32)
    jitter = 0.35 * jax.random.normal(key_jitter, (ROWS, EMB), jnp.float32)
    embeds = centers[members] + jitter
    return jnp.clip(embeds, -6.0, 6.0).astype(jnp.bfloat16)


def place_ends(result, own_key, least, high):
    longest = result.shape.index(max(result.shape))
    spots = []
    for shift in (0, 1):
        where = [jax.random.randint(jax.random.fold_in(own_key, axis), (), 0, length) for axis, length in enumerate(result.shape)]
        where[longest] = (where[longest] + shift) % result.shape[longest]
        spots.append(tuple(where))
    return result.at[spots[0]].set(least).at[spots[1]].set(high)


def centred(stream_key, extent, width, reach, kind=jnp.bfloat16):
    return jnp.clip(width * jax.random.normal(stream_key, extent, jnp.float32), -reach, reach).astype(kind)


def setup_inputs(seed: int = 0) -> dict:
    keys = jax.random.split(jax.random.key(seed), 6)
    embeds = draw_embeds(jax.random.fold_in(keys[5], 71), 0)
    w_hidden = centred(keys[1], (EMB, EMB), EMB ** -0.5, 0.3125)
    b_hidden = centred(keys[2], (EMB,), 0.5, 3.0, jnp.float32)
    w_out = centred(keys[3], (EMB, FEAT), EMB ** -0.5, 0.3125)
    probes = place_ends(jax.random.randint(keys[4], (PROBES, ROWS), 0, 2), jax.random.fold_in(keys[4], 1), 0, 1).astype(jnp.int32)
    return dict(embeds=embeds, w_hidden=w_hidden, b_hidden=b_hidden, w_out=w_out, probes=probes)


INV_WIDTH = 1.0 / 12.0
NOISE_LEVEL = 0.5
FLOOR_BETA = 0.01
EIGEN_FLOOR = 0.25

def rotate(matrix, vectors, first_idx, second_idx):
    diag_first = matrix[first_idx, first_idx]
    diag_second = matrix[second_idx, second_idx]
    off_value = matrix[first_idx, second_idx]
    half_angle = 0.5 * jnp.arctan2(2.0 * off_value, diag_first - diag_second)
    cosine = jnp.cos(half_angle)
    sine_val = jnp.sin(half_angle)
    row_first = matrix[first_idx]
    row_second = matrix[second_idx]
    matrix = matrix.at[first_idx].set(cosine * row_first + sine_val * row_second)
    matrix = matrix.at[second_idx].set(cosine * row_second - sine_val * row_first)
    col_first = matrix[:, first_idx]
    col_second = matrix[:, second_idx]
    matrix = matrix.at[:, first_idx].set(cosine * col_first + sine_val * col_second)
    matrix = matrix.at[:, second_idx].set(cosine * col_second - sine_val * col_first)
    vec_first = vectors[:, first_idx]
    vec_second = vectors[:, second_idx]
    vectors = vectors.at[:, first_idx].set(cosine * vec_first + sine_val * vec_second)
    vectors = vectors.at[:, second_idx].set(cosine * vec_second - sine_val * vec_first)
    return (matrix, vectors)

def quadrature(alphas, betas):
    tri_order = alphas.shape[0]
    identity = jnp.eye(tri_order, dtype=jnp.float32)
    upper_band = jnp.concatenate([jnp.zeros_like(alphas[:1]), betas], axis=0)
    shifted = jnp.eye(tri_order, k=1, dtype=jnp.float32)[:, :, None] * upper_band[None, :, :]
    matrix = identity[:, :, None] * alphas[None, :, :] + shifted + jnp.transpose(shifted, (1, 0, 2))
    vectors = jnp.broadcast_to(identity[:, :, None], matrix.shape) + jnp.zeros_like(matrix)
    for sweep_index in range(SWEEPS):
        for first_idx in range(tri_order):
            for second_idx in range(first_idx + 1, tri_order):
                matrix, vectors = rotate(matrix, vectors, first_idx, second_idx)
    eigenvalues = jnp.maximum(lax.optimization_barrier(jnp.sum(matrix * identity[:, :, None], axis=1)), EIGEN_FLOOR)
    leading = vectors[0]
    logdet = lax.optimization_barrier(jnp.sum(jnp.square(leading) * jnp.log(eigenvalues), axis=0))
    coefficients = lax.optimization_barrier(jnp.sum(vectors * (leading / eigenvalues)[None, :, :], axis=1))
    scale_grad = 1.0 - NOISE_LEVEL * coefficients[0]
    return (logdet, scale_grad, coefficients)

def apply_kernel(features, norms_all, vectors_low):
    total_rows = features.shape[0]
    block_rows = math.gcd(total_rows, 512)
    block_count = total_rows // block_rows
    feats_wide = features.astype(jnp.float32)
    vectors_wide = vectors_low.astype(jnp.float32)

    def one_block(block_index):
        row_block = lax.dynamic_slice_in_dim(feats_wide, block_index * block_rows, block_rows, 0)
        norm_block = lax.dynamic_slice_in_dim(norms_all, block_index * block_rows, block_rows, 0)
        inner = jnp.dot(row_block, feats_wide.T, precision=lax.Precision.HIGHEST)
        distance = norm_block[:, None] + norms_all[None, :] - 2.0 * inner
        kernel_low = jnp.exp(-jnp.maximum(distance, 0.0) * INV_WIDTH).astype(jnp.bfloat16)
        kernel_tile = lax.optimization_barrier(kernel_low).astype(jnp.float32)
        return jnp.dot(vectors_wide, kernel_tile.T, precision=lax.Precision.HIGHEST)
    stacked = lax.map(one_block, jnp.arange(block_count, dtype=jnp.int32))
    return jnp.transpose(stacked, (1, 0, 2)).reshape(vectors_low.shape[0], total_rows)

def reference(embeds, w_hidden, b_hidden, w_out, probes):
    hidden = jax.nn.gelu(jnp.dot(embeds, w_hidden, preferred_element_type=jnp.float32) + b_hidden).astype(jnp.bfloat16)
    features = jnp.dot(hidden, w_out, preferred_element_type=jnp.float32).astype(jnp.bfloat16)
    norms_all = lax.optimization_barrier(jnp.sum(jnp.square(features.astype(jnp.float32)), axis=1))
    scale_root = math.sqrt(ROWS)
    current = (2 * probes - 1).astype(jnp.float32) / scale_root
    previous = jnp.zeros_like(current)
    beta_prev = jnp.zeros((current.shape[0],), jnp.float32)
    basis_list = []
    alpha_list = []
    beta_list = []
    for iteration in range(ITERS):
        kernel_image = apply_kernel(features, norms_all, current.astype(jnp.bfloat16)) + NOISE_LEVEL * current
        alpha_now = lax.optimization_barrier(jnp.sum(current * kernel_image, axis=1))
        residual = kernel_image - alpha_now[:, None] * current - beta_prev[:, None] * previous
        basis_list.append(current)
        alpha_list.append(alpha_now)
        if iteration + 1 < ITERS:
            residual_sq = lax.optimization_barrier(jnp.sum(residual * residual, axis=1))
            beta_now = jnp.sqrt(jnp.maximum(residual_sq, 0.0) + FLOOR_BETA)
            beta_list.append(beta_now)
            previous = current
            current = residual / beta_now[:, None]
            beta_prev = beta_now
    logdet, scale_grad, coefficients = quadrature(jnp.stack(alpha_list), jnp.stack(beta_list))
    solves = scale_root * jnp.einsum('jp,jpn->pn', coefficients, jnp.stack(basis_list))
    return (solves, logdet, scale_grad)
```

```python
import functools
import math

import jax
import jax.numpy as jnp
from jax import lax
from jax.experimental import pallas as pl
from jax.experimental.pallas import tpu as pltpu
from jax.sharding import Mesh
from jax.sharding import PartitionSpec as P

ITERS = 8
SWEEPS = 6
GRP_ROW = ("grp", "row_0", "row_1", "row_2")

INV_WIDTH = 1.0 / 12.0
NOISE_LEVEL = 0.5
FLOOR_BETA = 0.01
EIGEN_FLOOR = 0.25
FIRST_GUESS = 1.0 + NOISE_LEVEL

BLOCK = 128
MESSAGE = 17
MESH_ID = pl.DeviceIdType.MESH


def far_first(sizes):
    def hops(offsets):
        return sum(min(o, n - o) for o, n in zip(offsets, sizes))

    every = [(i, j) for i in range(sizes[0]) for j in range(sizes[1])]
    return sorted(every[1:], key=hops, reverse=True)


def lanczos_kernel(
    dims,
    embeds,
    w_hidden,
    b_hidden,
    w_out,
    probes,
    basis,
    alphas,
    betas,
    feats_a,
    feats_b,
    row_norms,
    tile,
    gathered,
    lhs,
    part,
    arrived,
    send_fa,
    recv_fa,
    send_fb,
    recv_fb,
    send_a,
    recv_a,
    send_b,
    recv_b,
):
    ny, nx, nz, nc = dims
    na, nb = ny * nx, nz * nc
    probe_count = probes.shape[0]
    y, x, z, core = (lax.axis_index(name) for name in GRP_ROW)
    me_a = y * nx + x
    me_b = z * nc + core
    offsets_a = far_first((ny, nx))
    offsets_z = sorted(range(nz), key=lambda k: min(k, nz - k), reverse=True)

    def peer_a(ky, kx):
        return lax.rem(y + ky, ny), lax.rem(x + kx, nx)

    def source_a(ky, kx):
        return lax.rem(y + ny - ky, ny) * nx + lax.rem(x + nx - kx, nx)

    def targets_b(kz):
        there = lax.rem(z + kz, nz)
        if kz == 0:
            return [(there, 1 - core)]
        return [(there, c) for c in range(nc)]

    def sources_b(kz):
        there = lax.rem(z + nz - kz, nz)
        if kz == 0:
            return [(there, 1 - core)]
        return [(there, c) for c in range(nc)]

    barrier = pltpu.get_barrier_semaphore()
    for ky, kx in offsets_a:
        py, px = peer_a(ky, kx)
        pl.semaphore_signal(barrier, inc=1, device_id=(py, px, z, core), device_id_type=MESH_ID)
    for kz in offsets_z:
        for pz, pc in targets_b(kz):
            pl.semaphore_signal(barrier, inc=1, device_id=(y, x, pz, pc), device_id_type=MESH_ID)

    hidden = jnp.dot(embeds[...], w_hidden[...], preferred_element_type=jnp.float32)
    hidden = jax.nn.gelu(hidden + b_hidden[...]).astype(jnp.bfloat16)
    features = jnp.dot(hidden, w_out[...], preferred_element_type=jnp.float32)
    features = features.astype(jnp.bfloat16)
    feats_a[me_a] = features
    feats_b[me_b] = features
    pl.semaphore_wait(barrier, na + nb - 2)

    def feat_copy_a(ky, kx, slot):
        py, px = peer_a(ky, kx)
        k = ky * nx + kx
        return pltpu.make_async_remote_copy(
            src_ref=feats_a.at[me_a],
            dst_ref=feats_a.at[slot],
            send_sem=send_fa.at[k],
            recv_sem=recv_fa.at[k],
            device_id=(py, px, z, core),
            device_id_type=MESH_ID,
        )

    def feat_copy_b(kz, target, slot, sender):
        pz, pc = target
        return pltpu.make_async_remote_copy(
            src_ref=feats_b.at[me_b],
            dst_ref=feats_b.at[slot],
            send_sem=send_fb.at[kz * nc + pc],
            recv_sem=recv_fb.at[kz * nc + sender],
            device_id=(y, x, pz, pc),
            device_id_type=MESH_ID,
        )

    for kz in offsets_z:
        for target in targets_b(kz):
            feat_copy_b(kz, target, me_b, core).start()
    for ky, kx in offsets_a:
        feat_copy_a(ky, kx, me_a).start()
    for kz in offsets_z:
        for sz, sc in sources_b(kz):
            feat_copy_b(kz, (sz, sc), sz * nc + sc, sc).wait_recv()
    for ky, kx in offsets_a:
        feat_copy_a(ky, kx, source_a(ky, kx)).wait_recv()

    fold = -INV_WIDTH * math.log2(math.e)
    ones = jnp.ones((8, BLOCK), jnp.float32)
    width = nc * BLOCK
    for zi in range(nz):
        wide = feats_b[pl.ds(zi * nc, nc)].reshape(width, BLOCK).astype(jnp.float32)
        row_norms[:, zi * width : (zi + 1) * width] = fold * lax.dot_general(
            ones,
            wide * wide,
            (((1,), (1,)), ((), ())),
            precision=lax.Precision.HIGHEST,
            preferred_element_type=jnp.float32,
        )

    @pl.loop(0, na)
    def _(ai):
        cols = feats_a[ai]
        wide = cols.astype(jnp.float32)
        norm = fold * jnp.sum(wide * wide, axis=1, keepdims=True)
        for zi in range(nz):
            rows = feats_b[pl.ds(zi * nc, nc)].reshape(width, BLOCK)
            inner = lax.dot_general(
                cols, rows, (((1,), (1,)), ((), ())), preferred_element_type=jnp.float32
            )
            span = slice(zi * width, (zi + 1) * width)
            power = jnp.minimum((norm + row_norms[0:1, span]) - (2.0 * fold) * inner, 0.0)
            at = pl.ds(pl.multiple_of(ai * BLOCK, BLOCK), BLOCK)
            tile[at, span] = jnp.exp2(power).astype(jnp.bfloat16)

    lane = lax.broadcasted_iota(jnp.int32, (probe_count, BLOCK), 1)
    sub = lax.broadcasted_iota(jnp.int32, (probe_count, BLOCK), 0)

    def to_row(columns):
        spread = jnp.zeros((probe_count, BLOCK), jnp.float32)
        for i, column in enumerate(columns):
            spread = jnp.where(lane == i * probe_count + sub, column, spread)
        return jnp.sum(spread, axis=0, keepdims=True)

    def from_row(row, count):
        return [
            jnp.sum(jnp.where(lane == i * probe_count + sub, row, 0.0), axis=1, keepdims=True)
            for i in range(count)
        ]

    def copy_a(ky, kx, par, slot):
        py, px = peer_a(ky, kx)
        k = ky * nx + kx
        return pltpu.make_async_remote_copy(
            src_ref=gathered.at[par, me_a, pl.ds(0, MESSAGE)],
            dst_ref=gathered.at[par, slot, pl.ds(0, MESSAGE)],
            send_sem=send_a.at[k],
            recv_sem=recv_a.at[par, k],
            device_id=(py, px, z, core),
            device_id_type=MESH_ID,
        )

    def copy_b(kz, target, par, slot, sender):
        pz, pc = target
        return pltpu.make_async_remote_copy(
            src_ref=part.at[pz * nc + pc, pl.ds(0, MESSAGE)],
            dst_ref=arrived.at[par, slot, pl.ds(0, MESSAGE)],
            send_sem=send_b.at[kz * nc + pc],
            recv_sem=recv_b.at[par, kz * nc + sender],
            device_id=(y, x, pz, pc),
            device_id_type=MESH_ID,
        )

    def gather(par, vector, sums):
        gathered[par, me_a, 0:probe_count] = vector
        gathered[par, me_a, probe_count:MESSAGE] = sums
        for ky, kx in offsets_a:
            copy_a(ky, kx, par, me_a).start()
        for ky, kx in offsets_a:
            copy_a(ky, kx, par, source_a(ky, kx)).wait_recv()
        return jnp.sum(gathered[par, :, probe_count:MESSAGE], axis=0)

    def finish(par):
        for kz in offsets_z:
            for sz, sc in sources_b(kz):
                copy_b(kz, (sz, sc), par, sz * nc + sc, sc).wait_recv()
        for ky, kx in offsets_a:
            copy_a(ky, kx, par, me_a).wait_send()
        for kz in offsets_z:
            for target in targets_b(kz):
                copy_b(kz, target, par, me_b, core).wait_send()

    def spread(kz, par, block, sums):
        there = lax.rem(z + kz, nz)
        for c in range(nc):
            if block is not None:
                part[there * nc + c, 0:probe_count] = block[:, c * BLOCK : (c + 1) * BLOCK]
            part[there * nc + c, probe_count:MESSAGE] = sums
        for target in targets_b(kz):
            copy_b(kz, target, par, me_b, core).start()

    def matvec(par, sums):
        for ai in range(na):
            value = gathered[par, ai, 0:probe_count]
            high = value.astype(jnp.bfloat16)
            low = (value - high.astype(jnp.float32)).astype(jnp.bfloat16)
            lhs[0:probe_count, ai * BLOCK : (ai + 1) * BLOCK] = high
            lhs[probe_count:, ai * BLOCK : (ai + 1) * BLOCK] = low
        for kz in offsets_z:
            there = lax.rem(z + kz, nz)
            span = pl.ds(pl.multiple_of(there * width, width), width)
            both = jnp.dot(lhs[...], tile[:, span], preferred_element_type=jnp.float32)
            spread(kz, par, both[0:probe_count] + both[probe_count:], sums)

    def scalars(total, guess):
        alpha, ss, sq, qq = from_row(total, 4)
        shift = alpha - guess
        square = ss - 2.0 * shift * sq + shift * shift * qq
        return alpha, shift, jnp.sqrt(jnp.maximum(square, 0.0) + FLOOR_BETA)

    total_rows = na * nb * BLOCK
    start = (2 * probes[...] - 1).astype(jnp.float32) / math.sqrt(total_rows)
    zeros = jnp.zeros_like(start)
    column = jnp.zeros((probe_count, 1), jnp.float32)

    def step(j, carry):
        sent, last_q, last_w, guess, sums = carry
        par = lax.rem(j, 2)
        sums = gather(par, sent, sums)
        matvec(par, sums)
        finish(par)
        arrived[par, me_b] = part[me_b]
        received = jnp.sum(arrived[par], axis=0)
        image = received[0:probe_count] + NOISE_LEVEL * sent
        alpha, shift, beta = scalars(received[probe_count:MESSAGE], guess)
        first = j == 0
        alpha = jnp.where(first, FIRST_GUESS, alpha)
        shift = jnp.where(first, 0.0, shift)
        beta = jnp.where(first, 1.0, beta)
        q = (sent - shift * last_q) / beta
        w = (image - shift * last_w) / beta
        basis[j] = q
        before = lax.rem(j + ITERS - 1, ITERS)
        alphas[before] = to_row([alpha])
        betas[before] = to_row([beta])
        sent = w - alpha * q - beta * last_q
        sums = to_row(
            [
                jnp.sum(q * w, axis=1, keepdims=True),
                jnp.sum(sent * sent, axis=1, keepdims=True),
                jnp.sum(sent * q, axis=1, keepdims=True),
                jnp.sum(q * q, axis=1, keepdims=True),
            ]
        )
        return sent, q, w, alpha, sums

    none = jnp.zeros((1, BLOCK), jnp.float32)
    carry = lax.fori_loop(0, ITERS, step, (start, zeros, zeros, column, none))
    par = ITERS % 2
    sums = gather(par, carry[0], carry[4])
    for kz in offsets_z:
        spread(kz, par, None, sums)
    finish(par)
    arrived[par, me_b] = part[me_b]
    total = jnp.sum(arrived[par, :, probe_count:MESSAGE], axis=0)
    alphas[ITERS - 1] = to_row(from_row(total, 1))
    for ky, kx in offsets_a:
        feat_copy_a(ky, kx, me_a).wait_send()
    for kz in offsets_z:
        for target in targets_b(kz):
            feat_copy_b(kz, target, me_b, core).wait_send()


def rounds_of(order):
    ring = list(range(1, order))
    result = []
    for _ in range(order - 1):
        line = [0] + ring
        pairs = [(line[i], line[order - 1 - i]) for i in range(order // 2)]
        result.append([(min(p), max(p)) for p in pairs])
        ring = ring[1:] + ring[:1]
    return result


def rotation(first, second, off):
    gap = first - second
    double = 2.0 * off
    scale = jnp.maximum(jnp.abs(gap), jnp.abs(double))
    flat = scale == 0.0
    inverse = 1.0 / jnp.where(flat, 1.0, scale)
    gap = jnp.where(flat, 1.0, gap * inverse)
    double = double * inverse
    norm_inv = lax.rsqrt(gap * gap + double * double)
    cos_two = gap * norm_inv
    sin_two = double * norm_inv
    large = jnp.sqrt(0.5 + 0.5 * jnp.abs(cos_two))
    small = 0.5 * jnp.abs(sin_two) / large
    straight = gap >= 0.0
    cosine = jnp.where(straight, large, small)
    sine = jnp.where(straight, small, large)
    return cosine, jnp.where(double < 0.0, -sine, sine)


def quadrature_kernel(scale_root, basis, alphas, betas, solves, logdet, scale_grad):
    order = basis.shape[0]
    shape = (order, BLOCK)
    index = lax.broadcasted_iota(jnp.int32, shape, 0)
    diag = [jnp.broadcast_to(alphas[i], shape) for i in range(order)]
    off = {}
    for i in range(order):
        for j in range(i + 1, order):
            near = j == i + 1
            off[i, j] = jnp.broadcast_to(betas[i], shape) if near else jnp.zeros(shape, jnp.float32)
    vectors = [jnp.where(index == i, 1.0, 0.0).astype(jnp.float32) for i in range(order)]
    keys = sorted(off)

    def sweep(_, state):
        diag, entries, vectors = list(state[0]), dict(zip(keys, state[1])), list(state[2])

        def key(i, j):
            return (i, j) if i < j else (j, i)

        for pairs in rounds_of(order):
            turns = [rotation(diag[p], diag[q], entries[p, q]) for p, q in pairs]
            for (p, q), (c, s) in zip(pairs, turns):
                for k in range(order):
                    if k != p and k != q:
                        one, two = entries[key(p, k)], entries[key(q, k)]
                        entries[key(p, k)] = c * one + s * two
                        entries[key(q, k)] = c * two - s * one
                one, two, cross = diag[p], diag[q], entries[p, q]
                both = 2.0 * c * s * cross
                diag[p] = c * c * one + both + s * s * two
                diag[q] = s * s * one - both + c * c * two
                entries[p, q] = c * s * (two - one) + (c * c - s * s) * cross
                one, two = vectors[p], vectors[q]
                vectors[p] = c * one + s * two
                vectors[q] = c * two - s * one
        return tuple(diag), tuple(entries[k] for k in keys), tuple(vectors)

    state = (tuple(diag), tuple(off[k] for k in keys), tuple(vectors))
    diag, _, vectors = lax.fori_loop(0, SWEEPS, sweep, state)
    log_sum = jnp.zeros(shape, jnp.float32)
    coef = jnp.zeros(shape, jnp.float32)
    for k in range(order):
        value = jnp.maximum(diag[k], EIGEN_FLOOR)
        leading = jnp.broadcast_to(vectors[k][0:1], shape)
        log_sum = log_sum + leading * leading * jnp.log(value)
        coef = coef + vectors[k] * (leading / value)
    probe_count = basis.shape[1]
    logdet[...] = log_sum[0:1, 0:probe_count]
    scale_grad[...] = (1.0 - NOISE_LEVEL * coef)[0:1, 0:probe_count]
    lane = lax.broadcasted_iota(jnp.int32, (probe_count, BLOCK), 1)
    sub = lax.broadcasted_iota(jnp.int32, (probe_count, BLOCK), 0)
    total = jnp.zeros((probe_count, BLOCK), jnp.float32)
    for j in range(order):
        weight = jnp.sum(jnp.where(lane == sub, coef[j : j + 1], 0.0), axis=1, keepdims=True)
        total = total + weight * basis[j]
    solves[...] = scale_root * total


def local(dims, embeds, w_hidden, b_hidden, w_out, probes):
    ny, nx, nz, nc = dims
    na, nb = ny * nx, nz * nc
    rows, emb = embeds.shape
    probe_count = probes.shape[0]
    feat = w_out.shape[1]
    vmem = pl.BlockSpec(memory_space=pltpu.VMEM)
    row = jax.ShapeDtypeStruct((ITERS, 1, BLOCK), jnp.float32)
    basis, alphas, betas = pl.pallas_call(
        functools.partial(lanczos_kernel, dims),
        out_shape=(jax.ShapeDtypeStruct((ITERS, probe_count, rows), jnp.float32), row, row),
        in_specs=[vmem] * 5,
        out_specs=(vmem,) * 3,
        scratch_shapes=[
            pltpu.VMEM((na, rows, feat), jnp.bfloat16),
            pltpu.VMEM((nb, rows, feat), jnp.bfloat16),
            pltpu.VMEM((8, nb * rows), jnp.float32),
            pltpu.VMEM((na * rows, nb * rows), jnp.bfloat16),
            pltpu.VMEM((2, na, 24, rows), jnp.float32),
            pltpu.VMEM((2 * probe_count, na * rows), jnp.bfloat16),
            pltpu.VMEM((nb, 24, rows), jnp.float32),
            pltpu.VMEM((2, nb, 24, rows), jnp.float32),
            pltpu.SemaphoreType.DMA((na,)),
            pltpu.SemaphoreType.DMA((na,)),
            pltpu.SemaphoreType.DMA((nb,)),
            pltpu.SemaphoreType.DMA((nb,)),
            pltpu.SemaphoreType.DMA((na,)),
            pltpu.SemaphoreType.DMA((2, na)),
            pltpu.SemaphoreType.DMA((nb,)),
            pltpu.SemaphoreType.DMA((2, nb)),
        ],
        compiler_params=pltpu.CompilerParams(
            collective_id=0, has_side_effects=True, vmem_limit_bytes=48 * 1024 * 1024
        ),
        name="lanczos",
    )(embeds, w_hidden, b_hidden.reshape(1, emb), w_out, probes)
    scale_root = math.sqrt(na * nb * rows)
    small = jax.ShapeDtypeStruct((1, probe_count), jnp.float32)
    solves, logdet, scale_grad = pl.pallas_call(
        functools.partial(quadrature_kernel, scale_root),
        out_shape=(jax.ShapeDtypeStruct((probe_count, rows), jnp.float32), small, small),
        in_specs=[vmem] * 3,
        out_specs=(vmem,) * 3,
        name="quadrature",
    )(basis, alphas, betas)
    return solves, logdet.reshape(probe_count), scale_grad.reshape(probe_count)


def solution(mesh):
    cores = 2
    ny = mesh.shape["grp"]
    nx = 4
    dims = (ny, nx, mesh.shape["row"] // (nx * cores), cores)
    finer = Mesh(mesh.devices.reshape(dims), GRP_ROW)
    return jax.shard_map(
        functools.partial(local, dims),
        mesh=finer,
        in_specs=(P(GRP_ROW, None), P(), P(), P(), P(None, GRP_ROW)),
        out_specs=(P(None, GRP_ROW), P(), P()),
        check_vma=False,
    )
```

```python
import functools
import math

import jax
import jax.numpy as jnp
from jax import lax
from jax.experimental import pallas as pl
from jax.experimental.pallas import tpu as pltpu
from jax.sharding import Mesh
from jax.sharding import PartitionSpec as P

ITERS = 8
SWEEPS = 6
GRP_ROW = ("grp", "row_0", "row_1", "row_2")

INV_WIDTH = 1.0 / 12.0
NOISE_LEVEL = 0.5
FLOOR_BETA = 0.01
EIGEN_FLOOR = 0.25
FIRST_GUESS = 1.0 + NOISE_LEVEL

BLOCK = 128
MESSAGE = 17
MESH_ID = pl.DeviceIdType.MESH


def far_first(sizes):
    def hops(offsets):
        return sum(min(o, n - o) for o, n in zip(offsets, sizes))

    every = [(i, j) for i in range(sizes[0]) for j in range(sizes[1])]
    return sorted(every[1:], key=hops, reverse=True)


def lanczos_kernel(
    dims,
    embeds_in,
    w_hidden_in,
    b_hidden_in,
    w_out_in,
    probes_in,
    out,
    embeds,
    w_hidden,
    b_hidden,
    w_out,
    probes,
    feats_a,
    feats_b,
    row_norms,
    tile,
    gathered,
    lhs,
    part,
    arrived,
    line,
    load_sems,
    send_fa,
    recv_fa,
    send_fb,
    recv_fb,
    send_pass,
    recv_pass,
    send_a,
    recv_a,
    send_b,
    recv_b,
    send_line,
    recv_line,
):
    ny, nx, nz, nc = dims
    na, nb = ny * nx, nz * nc
    probe_count = probes.shape[0]
    y, x, z, core = (lax.axis_index(name) for name in GRP_ROW)
    me_a = y * nx + x
    me_b = z * nc + core
    other = 1 - core
    offsets_a = far_first((ny, nx))
    offsets_z = sorted(range(nz), key=lambda k: min(k, nz - k), reverse=True)
    near_z = offsets_z[::-1]

    def peer_a(ky, kx):
        return lax.rem(y + ky, ny), lax.rem(x + kx, nx)

    def source_a(ky, kx):
        return lax.rem(y + ny - ky, ny) * nx + lax.rem(x + nx - kx, nx)

    def ahead(kz):
        return lax.rem(z + kz, nz)

    def behind(kz):
        return lax.rem(z + nz - kz, nz)

    def partners(there, kz):
        return [(there, other)] if kz == 0 else [(there, c) for c in range(nc)]

    loads = [
        pltpu.make_async_copy(source, target, load_sems.at[i])
        for i, (source, target) in enumerate(
            (
                (embeds_in, embeds),
                (w_hidden_in, w_hidden),
                (b_hidden_in, b_hidden.at[0]),
                (w_out_in, w_out),
                (probes_in, probes),
            )
        )
    ]
    for load in loads:
        load.start()

    barrier = pltpu.get_barrier_semaphore()
    for ky, kx in offsets_a:
        py, px = peer_a(ky, kx)
        pl.semaphore_signal(barrier, inc=1, device_id=(py, px, z, core), device_id_type=MESH_ID)
    for kz in offsets_z:
        for pz, pc in partners(ahead(kz), kz):
            pl.semaphore_signal(barrier, inc=1, device_id=(y, x, pz, pc), device_id_type=MESH_ID)

    lane = lax.broadcasted_iota(jnp.int32, (probe_count, BLOCK), 1)
    sub = lax.broadcasted_iota(jnp.int32, (probe_count, BLOCK), 0)

    def to_row(columns, base=0):
        spread = jnp.zeros((probe_count, BLOCK), jnp.float32)
        for i, column in enumerate(columns, base):
            spread = jnp.where(lane == i * probe_count + sub, column, spread)
        return jnp.sum(spread, axis=0, keepdims=True)

    def from_row(row, count):
        return [
            jnp.sum(jnp.where(lane == i * probe_count + sub, row, 0.0), axis=1, keepdims=True)
            for i in range(count)
        ]

    def total_of(left, right):
        return jnp.sum(left * right, axis=1, keepdims=True)

    whole = pl.ds(0, MESSAGE)
    vector_rows = pl.ds(0, probe_count)
    sums_row = pl.ds(probe_count, 1)

    def copy_a(ky, kx, par, slot, rows=whole):
        py, px = peer_a(ky, kx)
        k = ky * nx + kx
        return pltpu.make_async_remote_copy(
            src_ref=gathered.at[par, me_a, rows],
            dst_ref=gathered.at[par, slot, rows],
            send_sem=send_a.at[k],
            recv_sem=recv_a.at[par, k],
            device_id=(py, px, z, core),
            device_id_type=MESH_ID,
        )

    def copy_b(kz, target, par, slot, sender, rows=whole):
        pz, pc = target
        return pltpu.make_async_remote_copy(
            src_ref=part.at[pz * nc + pc, rows],
            dst_ref=arrived.at[par, slot, rows],
            send_sem=send_b.at[kz * nc + pc],
            recv_sem=recv_b.at[par, kz * nc + sender],
            device_id=(y, x, pz, pc),
            device_id_type=MESH_ID,
        )

    def copy_line(kz, target, slot, sender):
        pz, pc = target
        return pltpu.make_async_remote_copy(
            src_ref=line.at[me_b],
            dst_ref=line.at[slot],
            send_sem=send_line.at[kz * nc + pc],
            recv_sem=recv_line.at[kz * nc + sender],
            device_id=(y, x, pz, pc),
            device_id_type=MESH_ID,
        )

    def send_vector(par, vector, sums):
        gathered[par, me_a, 0:probe_count] = vector
        gathered[par, me_a, probe_count:MESSAGE] = sums
        for ky, kx in offsets_a:
            copy_a(ky, kx, par, me_a).start()

    def take_vectors(par):
        for ky, kx in offsets_a:
            copy_a(ky, kx, par, source_a(ky, kx)).wait_recv()
        return jnp.sum(gathered[par, :, probe_count:MESSAGE], axis=0)

    def sent_vector(par):
        for ky, kx in offsets_a:
            copy_a(ky, kx, par, me_a).wait_send()

    def take_parts(par, rows=whole):
        for kz in offsets_z:
            for sz, sc in partners(behind(kz), kz):
                copy_b(kz, (sz, sc), par, sz * nc + sc, sc, rows).wait_recv()

    def sent_parts(par, rows=whole):
        for kz in offsets_z:
            for target in partners(ahead(kz), kz):
                copy_b(kz, target, par, me_b, core, rows).wait_send()

    width = nc * BLOCK

    def split_vectors(par):
        for ai in range(na):
            value = gathered[par, ai, 0:probe_count]
            high = value.astype(jnp.bfloat16)
            low = (value - high.astype(jnp.float32)).astype(jnp.bfloat16)
            lhs[0:probe_count, ai * BLOCK : (ai + 1) * BLOCK] = high
            lhs[probe_count:, ai * BLOCK : (ai + 1) * BLOCK] = low

    def product(there):
        span = pl.ds(pl.multiple_of(there * width, width), width)
        both = jnp.dot(lhs[...], tile[:, span], preferred_element_type=jnp.float32)
        return both[0:probe_count] + both[probe_count:]

    total_rows = na * nb * BLOCK
    loads[4].wait()
    start = (2 * probes[...] - 1).astype(jnp.float32) / math.sqrt(total_rows)
    zeros = jnp.zeros_like(start)
    none = jnp.zeros((1, BLOCK), jnp.float32)

    for load in loads[:4]:
        load.wait()
    hidden = jnp.dot(embeds[...], w_hidden[...], preferred_element_type=jnp.float32)
    hidden = jax.nn.gelu(hidden + b_hidden[...]).astype(jnp.bfloat16)
    features = jnp.dot(hidden, w_out[...], preferred_element_type=jnp.float32)
    features = features.astype(jnp.bfloat16)
    feats_a[me_a] = features
    feats_b[me_b] = features

    def feat_copy_a(ky, kx, slot):
        py, px = peer_a(ky, kx)
        k = ky * nx + kx
        return pltpu.make_async_remote_copy(
            src_ref=feats_a.at[me_a],
            dst_ref=feats_a.at[slot],
            send_sem=send_fa.at[k],
            recv_sem=recv_fa.at[k],
            device_id=(py, px, z, core),
            device_id_type=MESH_ID,
        )

    def feat_copy_z(kz, there, slot):
        return pltpu.make_async_remote_copy(
            src_ref=feats_b.at[me_b],
            dst_ref=feats_b.at[slot],
            send_sem=send_fb.at[kz],
            recv_sem=recv_fb.at[kz],
            device_id=(y, x, there, core),
            device_id_type=MESH_ID,
        )

    def hand_over(kz, source_core, target_core):
        slot = feats_b.at[behind(kz) * nc + source_core]
        return pltpu.make_async_remote_copy(
            src_ref=slot,
            dst_ref=slot,
            send_sem=send_pass.at[kz],
            recv_sem=recv_pass.at[kz],
            device_id=(y, x, z, target_core),
            device_id_type=MESH_ID,
        )

    pl.semaphore_wait(barrier, na + nb - 2)
    for kz in near_z[1:]:
        feat_copy_z(kz, ahead(kz), me_b).start()
    hand_over(0, core, other).start()
    rows_a = [(0, 1), (ny - 1, 2)] if ny == 4 else [(ky,) for ky in range(ny)]
    near_a = [[(ky, kx) for ky in group for kx in range(nx)] for group in rows_a]
    for group in near_a:
        for ky, kx in group:
            if (ky, kx) != (0, 0):
                feat_copy_a(ky, kx, me_a).start()
    send_vector(0, start, none)

    fold = -INV_WIDTH * math.log2(math.e)
    ones = jnp.ones((8, BLOCK), jnp.float32)

    def take_columns(group):
        for ky, kx in group:
            if (ky, kx) != (0, 0):
                feat_copy_a(ky, kx, source_a(ky, kx)).wait_recv()

    def span_of(there):
        return pl.ds(pl.multiple_of(there * width, width), width)

    def rows_at(there):
        return feats_b[pl.ds(there * nc, nc)].reshape(width, BLOCK)

    def take_rows(group):
        for kz in group:
            if kz != 0:
                feat_copy_z(kz, behind(kz), behind(kz) * nc + core).wait_recv()
                hand_over(kz, core, other).start()
        for kz in group:
            hand_over(kz, other, other).wait_recv()
            wide = rows_at(behind(kz)).astype(jnp.float32)
            row_norms[:, span_of(behind(kz))] = fold * lax.dot_general(
                ones,
                wide * wide,
                (((1,), (1,)), ((), ())),
                precision=lax.Precision.HIGHEST,
                preferred_element_type=jnp.float32,
            )

    def fill(columns, rows):
        first_row = columns[0][0]
        row_step = columns[-1][0] - first_row

        @pl.loop(0, len(columns))
        def _(i):
            ai = source_a(first_row + row_step * (i // nx), lax.rem(i, nx))
            cols = feats_a[ai]
            wide = cols.astype(jnp.float32)
            norm = fold * jnp.sum(wide * wide, axis=1, keepdims=True)
            at = pl.ds(pl.multiple_of(ai * BLOCK, BLOCK), BLOCK)
            for kz in rows:
                there = behind(kz)
                span = span_of(there)
                inner = lax.dot_general(
                    cols,
                    rows_at(there),
                    (((1,), (1,)), ((), ())),
                    preferred_element_type=jnp.float32,
                )
                power = jnp.minimum((norm + row_norms[0:1, span]) - (2.0 * fold) * inner, 0.0)
                tile[at, span] = jnp.exp2(power).astype(jnp.bfloat16)

    half = nz // 2
    near_rows, far_rows = near_z[:half], near_z[half:]
    take_columns(near_a[0])
    take_rows(near_rows)
    fill(near_a[0], near_rows)
    take_columns(near_a[1])
    fill(near_a[1], near_rows)
    take_rows(far_rows)
    fill(near_a[0], far_rows)
    fill(near_a[1], far_rows)

    def scalars(total, guess):
        alpha, ss, sq, qq, sw = from_row(total, 5)
        shift = alpha - guess
        square = ss - 2.0 * shift * sq + shift * shift * qq
        return alpha, shift, jnp.sqrt(jnp.maximum(square, 0.0) + FLOOR_BETA), ss, sw

    def step(j, carry):
        sent, last_q, last_w, guess = carry
        par = lax.rem(j, 2)
        sums = take_vectors(par)
        split_vectors(par)
        for kz in offsets_z:
            there = ahead(kz)
            block = product(there)
            for c in range(nc):
                part[there * nc + c, 0:probe_count] = block[:, c * BLOCK : (c + 1) * BLOCK]
                part[there * nc + c, probe_count:MESSAGE] = sums
            for target in partners(there, kz):
                copy_b(kz, target, par, me_b, core).start()
        arrived[par, me_b] = part[me_b]
        take_parts(par)
        received = jnp.sum(arrived[par], axis=0)
        image = received[0:probe_count] + NOISE_LEVEL * sent
        alpha, shift, beta, _, _ = scalars(received[probe_count:MESSAGE], guess)
        first = j == 0
        alpha = jnp.where(first, FIRST_GUESS, alpha)
        shift = jnp.where(first, 0.0, shift)
        beta = jnp.where(first, 1.0, beta)
        q = (sent - shift * last_q) / beta
        w = (image - shift * last_w) / beta
        new = w - alpha * q - beta * last_q
        sums = to_row([total_of(q, w), total_of(new, new), total_of(new, q), total_of(q, q), total_of(new, w)])
        sent_vector(par)
        send_vector(1 - par, new, sums)
        sent_parts(par)
        out[j, 0:probe_count] = q
        before = lax.rem(j + ITERS - 1, ITERS)
        out[before, probe_count : probe_count + 1] = to_row([alpha])
        out[before, probe_count + 1 : probe_count + 2] = to_row([beta])
        return new, q, w, alpha

    column = jnp.zeros((probe_count, 1), jnp.float32)
    last = ITERS - 1
    sent, last_q, _, guess = lax.fori_loop(0, last, step, (start, zeros, zeros, column))
    par = last % 2
    line[me_b] = sent
    for kz in offsets_z:
        for target in partners(ahead(kz), kz):
            copy_line(kz, target, me_b, core).start()
    sums = take_vectors(par)
    split_vectors(par)
    for kz in offsets_z:
        for sz, sc in partners(behind(kz), kz):
            copy_line(kz, (sz, sc), sz * nc + sc, sc).wait_recv()
    products = zeros
    for zi in range(nz):
        block = product(zi)
        for c in range(nc):
            products = products + block[:, c * BLOCK : (c + 1) * BLOCK] * line[zi * nc + c]
    row = sums + to_row([jnp.sum(products, axis=1, keepdims=True)], 5)
    for bi in range(nb):
        part[bi, probe_count:MESSAGE] = row
    for kz in offsets_z:
        for target in partners(ahead(kz), kz):
            copy_b(kz, target, par, me_b, core, sums_row).start()
    arrived[par, me_b, probe_count:MESSAGE] = row
    take_parts(par, sums_row)
    total = jnp.sum(arrived[par, :, probe_count:MESSAGE], axis=0)
    sent_vector(par)
    free = 1 - par
    gathered[free, me_a, probe_count:MESSAGE] = total
    for ky, kx in offsets_a:
        copy_a(ky, kx, free, me_a, sums_row).start()
    alpha, shift, beta, ss, sw = scalars(total, guess)
    out[last, 0:probe_count] = (sent - shift * last_q) / beta
    out[last - 1, probe_count : probe_count + 1] = to_row([alpha])
    out[last - 1, probe_count + 1 : probe_count + 2] = to_row([beta])
    for ky, kx in offsets_a:
        copy_a(ky, kx, free, source_a(ky, kx), sums_row).wait_recv()
    form = from_row(jnp.sum(gathered[free, :, probe_count:MESSAGE], axis=0), 6)[5]
    form = form + NOISE_LEVEL * ss - 2.0 * shift * sw + shift * shift * alpha
    out[last, probe_count : probe_count + 1] = to_row([form / (beta * beta)])
    for ky, kx in offsets_a:
        copy_a(ky, kx, free, me_a, sums_row).wait_send()
        feat_copy_a(ky, kx, me_a).wait_send()
    sent_parts(par, sums_row)
    for kz in offsets_z:
        for target in partners(ahead(kz), kz):
            copy_line(kz, target, me_b, core).wait_send()
        hand_over(kz, core, other).wait_send()
        if kz != 0:
            feat_copy_z(kz, ahead(kz), me_b).wait_send()


def rounds_of(order):
    ring = list(range(1, order))
    result = []
    for _ in range(order - 1):
        line = [0] + ring
        pairs = [(line[i], line[order - 1 - i]) for i in range(order // 2)]
        result.append([(min(p), max(p)) for p in pairs])
        ring = ring[1:] + ring[:1]
    return result


def rotation(first, second, off):
    gap = first - second
    double = 2.0 * off
    scale = jnp.maximum(jnp.abs(gap), jnp.abs(double))
    flat = scale == 0.0
    inverse = 1.0 / jnp.where(flat, 1.0, scale)
    gap = jnp.where(flat, 1.0, gap * inverse)
    double = double * inverse
    norm_inv = lax.rsqrt(gap * gap + double * double)
    cos_two = gap * norm_inv
    sin_two = double * norm_inv
    large = jnp.sqrt(0.5 + 0.5 * jnp.abs(cos_two))
    small = 0.5 * jnp.abs(sin_two) / large
    straight = gap >= 0.0
    cosine = jnp.where(straight, large, small)
    sine = jnp.where(straight, small, large)
    return cosine, jnp.where(double < 0.0, -sine, sine)


def quadrature_kernel(scale_root, lanczos, solves, logdet, scale_grad):
    order, probe_count = lanczos.shape[0], solves.shape[0]
    shape = (order, BLOCK)
    index = lax.broadcasted_iota(jnp.int32, shape, 0)
    diag = [jnp.broadcast_to(lanczos[i, probe_count : probe_count + 1], shape) for i in range(order)]
    off = {}
    for i in range(order):
        for j in range(i + 1, order):
            near = j == i + 1
            band = lanczos[i, probe_count + 1 : probe_count + 2] if near else 0.0
            off[i, j] = jnp.broadcast_to(band, shape)
    vectors = [jnp.where(index == i, 1.0, 0.0).astype(jnp.float32) for i in range(order)]
    keys = sorted(off)

    def sweep(_, state):
        diag, entries, vectors = list(state[0]), dict(zip(keys, state[1])), list(state[2])

        def key(i, j):
            return (i, j) if i < j else (j, i)

        for pairs in rounds_of(order):
            turns = [rotation(diag[p], diag[q], entries[p, q]) for p, q in pairs]
            for (p, q), (c, s) in zip(pairs, turns):
                for k in range(order):
                    if k != p and k != q:
                        one, two = entries[key(p, k)], entries[key(q, k)]
                        entries[key(p, k)] = c * one + s * two
                        entries[key(q, k)] = c * two - s * one
                one, two, cross = diag[p], diag[q], entries[p, q]
                both = 2.0 * c * s * cross
                diag[p] = c * c * one + both + s * s * two
                diag[q] = s * s * one - both + c * c * two
                entries[p, q] = c * s * (two - one) + (c * c - s * s) * cross
                one, two = vectors[p], vectors[q]
                vectors[p] = c * one + s * two
                vectors[q] = c * two - s * one
        return tuple(diag), tuple(entries[k] for k in keys), tuple(vectors)

    state = (tuple(diag), tuple(off[k] for k in keys), tuple(vectors))
    diag, _, vectors = lax.fori_loop(0, SWEEPS, sweep, state)
    log_sum = jnp.zeros(shape, jnp.float32)
    coef = jnp.zeros(shape, jnp.float32)
    for k in range(order):
        value = jnp.maximum(diag[k], EIGEN_FLOOR)
        leading = jnp.broadcast_to(vectors[k][0:1], shape)
        log_sum = log_sum + leading * leading * jnp.log(value)
        coef = coef + vectors[k] * (leading / value)
    logdet[...] = log_sum[0:1, 0:probe_count]
    scale_grad[...] = (1.0 - NOISE_LEVEL * coef)[0:1, 0:probe_count]
    lane = lax.broadcasted_iota(jnp.int32, (probe_count, BLOCK), 1)
    sub = lax.broadcasted_iota(jnp.int32, (probe_count, BLOCK), 0)
    total = jnp.zeros((probe_count, BLOCK), jnp.float32)
    for j in range(order):
        weight = jnp.sum(jnp.where(lane == sub, coef[j : j + 1], 0.0), axis=1, keepdims=True)
        total = total + weight * lanczos[j, 0:probe_count]
    solves[...] = scale_root * total


def local(dims, embeds, w_hidden, b_hidden, w_out, probes):
    ny, nx, nz, nc = dims
    na, nb = ny * nx, nz * nc
    rows, emb = embeds.shape
    probe_count = probes.shape[0]
    feat = w_out.shape[1]
    vmem = pl.BlockSpec(memory_space=pltpu.VMEM)
    hbm = pl.BlockSpec(memory_space=pltpu.HBM)
    lanczos = pl.pallas_call(
        functools.partial(lanczos_kernel, dims),
        out_shape=jax.ShapeDtypeStruct((ITERS, 24, rows), jnp.float32),
        in_specs=[hbm] * 5,
        out_specs=vmem,
        scratch_shapes=[
            pltpu.VMEM((rows, emb), jnp.bfloat16),
            pltpu.VMEM((emb, emb), jnp.bfloat16),
            pltpu.VMEM((1, emb), jnp.float32),
            pltpu.VMEM((emb, feat), jnp.bfloat16),
            pltpu.VMEM((probe_count, rows), jnp.int32),
            pltpu.VMEM((na, rows, feat), jnp.bfloat16),
            pltpu.VMEM((nb, rows, feat), jnp.bfloat16),
            pltpu.VMEM((8, nb * rows), jnp.float32),
            pltpu.VMEM((na * rows, nb * rows), jnp.bfloat16),
            pltpu.VMEM((2, na, 24, rows), jnp.float32),
            pltpu.VMEM((2 * probe_count, na * rows), jnp.bfloat16),
            pltpu.VMEM((nb, 24, rows), jnp.float32),
            pltpu.VMEM((2, nb, 24, rows), jnp.float32),
            pltpu.VMEM((nb, probe_count, rows), jnp.float32),
            pltpu.SemaphoreType.DMA((5,)),
            pltpu.SemaphoreType.DMA((na,)),
            pltpu.SemaphoreType.DMA((na,)),
            pltpu.SemaphoreType.DMA((nz,)),
            pltpu.SemaphoreType.DMA((nz,)),
            pltpu.SemaphoreType.DMA((nz,)),
            pltpu.SemaphoreType.DMA((nz,)),
            pltpu.SemaphoreType.DMA((na,)),
            pltpu.SemaphoreType.DMA((2, na)),
            pltpu.SemaphoreType.DMA((nb,)),
            pltpu.SemaphoreType.DMA((2, nb)),
            pltpu.SemaphoreType.DMA((nb,)),
            pltpu.SemaphoreType.DMA((nb,)),
        ],
        compiler_params=pltpu.CompilerParams(
            collective_id=0, has_side_effects=True, vmem_limit_bytes=48 * 1024 * 1024
        ),
        name="lanczos",
    )(embeds, w_hidden, b_hidden, w_out, probes)
    scale_root = math.sqrt(na * nb * rows)
    small = jax.ShapeDtypeStruct((1, probe_count), jnp.float32)
    solves, logdet, scale_grad = pl.pallas_call(
        functools.partial(quadrature_kernel, scale_root),
        out_shape=(jax.ShapeDtypeStruct((probe_count, rows), jnp.float32), small, small),
        in_specs=[vmem],
        out_specs=(vmem,) * 3,
        name="quadrature",
    )(lanczos)
    return solves, logdet.reshape(probe_count), scale_grad.reshape(probe_count)


def solution(mesh):
    cores = 2
    ny = mesh.shape["grp"]
    nx = 4
    dims = (ny, nx, mesh.shape["row"] // (nx * cores), cores)
    finer = Mesh(mesh.devices.reshape(dims), GRP_ROW)
    return jax.shard_map(
        functools.partial(local, dims),
        mesh=finer,
        in_specs=(P(GRP_ROW, None), P(), P(), P(), P(None, GRP_ROW)),
        out_specs=(P(None, GRP_ROW), P(), P()),
        check_vma=False,
    )
```

```python
import functools
import math

import jax
import jax.numpy as jnp
from jax import lax
from jax.experimental import pallas as pl
from jax.experimental.pallas import tpu as pltpu
from jax.sharding import Mesh
from jax.sharding import PartitionSpec as P

ITERS = 8
SWEEPS = 6
GRP_ROW = ("grp", "row_0", "row_1", "row_2")

INV_WIDTH = 1.0 / 12.0
NOISE_LEVEL = 0.5
FLOOR_BETA = 0.01
EIGEN_FLOOR = 0.25
FIRST_GUESS = 1.0 + NOISE_LEVEL

BLOCK = 128
MESSAGE = 17
MESH_ID = pl.DeviceIdType.MESH


def far_first(sizes):
    def hops(offsets):
        return sum(min(o, n - o) for o, n in zip(offsets, sizes))

    every = [(i, j) for i in range(sizes[0]) for j in range(sizes[1])]
    return sorted(every[1:], key=hops, reverse=True)


def lanczos_kernel(
    dims,
    embeds_in,
    w_hidden_in,
    b_hidden_in,
    w_out_in,
    probes_in,
    out,
    embeds,
    w_hidden,
    b_hidden,
    w_out,
    probes,
    feats_a,
    feats_b,
    row_norms,
    tile,
    gathered,
    lhs,
    part,
    arrived,
    line,
    load_sems,
    send_fa,
    recv_fa,
    send_fb,
    recv_fb,
    send_pass,
    recv_pass,
    send_a,
    recv_a,
    send_b,
    recv_b,
    send_line,
    recv_line,
):
    ny, nx, nz, nc = dims
    na, nb = ny * nx, nz * nc
    probe_count = probes.shape[0]
    y, x, z, core = (lax.axis_index(name) for name in GRP_ROW)
    me_a = y * nx + x
    me_b = z * nc + core
    other = 1 - core
    offsets_a = far_first((ny, nx))
    offsets_z = sorted(range(nz), key=lambda k: min(k, nz - k), reverse=True)
    near_z = offsets_z[::-1]

    def peer_a(ky, kx):
        return lax.rem(y + ky, ny), lax.rem(x + kx, nx)

    def source_a(ky, kx):
        return lax.rem(y + ny - ky, ny) * nx + lax.rem(x + nx - kx, nx)

    def ahead(kz):
        return lax.rem(z + kz, nz)

    def behind(kz):
        return lax.rem(z + nz - kz, nz)

    def partners(there, kz):
        return [(there, other)] if kz == 0 else [(there, c) for c in range(nc)]

    loads = [
        pltpu.make_async_copy(source, target, load_sems.at[i])
        for i, (source, target) in enumerate(
            (
                (embeds_in, embeds),
                (w_hidden_in, w_hidden),
                (b_hidden_in, b_hidden.at[0]),
                (w_out_in, w_out),
                (probes_in, probes),
            )
        )
    ]
    for load in loads:
        load.start()

    barrier = pltpu.get_barrier_semaphore()
    for ky, kx in offsets_a:
        py, px = peer_a(ky, kx)
        pl.semaphore_signal(barrier, inc=1, device_id=(py, px, z, core), device_id_type=MESH_ID)
    for kz in offsets_z:
        for pz, pc in partners(ahead(kz), kz):
            pl.semaphore_signal(barrier, inc=1, device_id=(y, x, pz, pc), device_id_type=MESH_ID)

    lane = lax.broadcasted_iota(jnp.int32, (probe_count, BLOCK), 1)
    sub = lax.broadcasted_iota(jnp.int32, (probe_count, BLOCK), 0)

    def to_row(columns, base=0):
        spread = jnp.zeros((probe_count, BLOCK), jnp.float32)
        for i, column in enumerate(columns, base):
            spread = jnp.where(lane == i * probe_count + sub, column, spread)
        return jnp.sum(spread, axis=0, keepdims=True)

    def from_row(row, count):
        return [
            jnp.sum(jnp.where(lane == i * probe_count + sub, row, 0.0), axis=1, keepdims=True)
            for i in range(count)
        ]

    def total_of(left, right):
        return jnp.sum(left * right, axis=1, keepdims=True)

    whole = pl.ds(0, MESSAGE)
    vector_rows = pl.ds(0, probe_count)
    sums_row = pl.ds(probe_count, 1)

    def copy_a(ky, kx, par, slot, rows=whole):
        py, px = peer_a(ky, kx)
        k = ky * nx + kx
        return pltpu.make_async_remote_copy(
            src_ref=gathered.at[par, me_a, rows],
            dst_ref=gathered.at[par, slot, rows],
            send_sem=send_a.at[k],
            recv_sem=recv_a.at[par, k],
            device_id=(py, px, z, core),
            device_id_type=MESH_ID,
        )

    def copy_b(kz, target, par, slot, sender, rows=whole):
        pz, pc = target
        return pltpu.make_async_remote_copy(
            src_ref=part.at[pz * nc + pc, rows],
            dst_ref=arrived.at[par, slot, rows],
            send_sem=send_b.at[kz * nc + pc],
            recv_sem=recv_b.at[par, kz * nc + sender],
            device_id=(y, x, pz, pc),
            device_id_type=MESH_ID,
        )

    def copy_line(kz, target, slot, sender):
        pz, pc = target
        return pltpu.make_async_remote_copy(
            src_ref=line.at[me_b],
            dst_ref=line.at[slot],
            send_sem=send_line.at[kz * nc + pc],
            recv_sem=recv_line.at[kz * nc + sender],
            device_id=(y, x, pz, pc),
            device_id_type=MESH_ID,
        )

    def send_vector(par, vector, sums):
        gathered[par, me_a, 0:probe_count] = vector
        gathered[par, me_a, probe_count:MESSAGE] = sums
        for ky, kx in offsets_a:
            copy_a(ky, kx, par, me_a).start()

    def take_vectors(par):
        for ky, kx in offsets_a:
            copy_a(ky, kx, par, source_a(ky, kx)).wait_recv()
        return jnp.sum(gathered[par, :, probe_count:MESSAGE], axis=0)

    def sent_vector(par):
        for ky, kx in offsets_a:
            copy_a(ky, kx, par, me_a).wait_send()

    def take_parts(par, rows=whole):
        for kz in offsets_z:
            for sz, sc in partners(behind(kz), kz):
                copy_b(kz, (sz, sc), par, sz * nc + sc, sc, rows).wait_recv()

    def sent_parts(par, rows=whole):
        for kz in offsets_z:
            for target in partners(ahead(kz), kz):
                copy_b(kz, target, par, me_b, core, rows).wait_send()

    width = nc * BLOCK

    def split_vectors(par):
        for ai in range(na):
            value = gathered[par, ai, 0:probe_count]
            high = value.astype(jnp.bfloat16)
            low = (value - high.astype(jnp.float32)).astype(jnp.bfloat16)
            lhs[0:probe_count, ai * BLOCK : (ai + 1) * BLOCK] = high
            lhs[probe_count:, ai * BLOCK : (ai + 1) * BLOCK] = low

    def product(there):
        span = pl.ds(pl.multiple_of(there * width, width), width)
        both = jnp.dot(lhs[...], tile[:, span], preferred_element_type=jnp.float32)
        return both[0:probe_count] + both[probe_count:]

    total_rows = na * nb * BLOCK
    loads[4].wait()
    start = (2 * probes[...] - 1).astype(jnp.float32) / math.sqrt(total_rows)
    zeros = jnp.zeros_like(start)
    none = jnp.zeros((1, BLOCK), jnp.float32)

    for load in loads[:4]:
        load.wait()
    hidden = jnp.dot(embeds[...], w_hidden[...], preferred_element_type=jnp.float32)
    hidden = jax.nn.gelu(hidden + b_hidden[...]).astype(jnp.bfloat16)
    features = jnp.dot(hidden, w_out[...], preferred_element_type=jnp.float32)
    features = features.astype(jnp.bfloat16)
    feats_a[me_a] = features
    feats_b[me_b] = features

    def feat_copy_a(ky, kx, slot):
        py, px = peer_a(ky, kx)
        k = ky * nx + kx
        return pltpu.make_async_remote_copy(
            src_ref=feats_a.at[me_a],
            dst_ref=feats_a.at[slot],
            send_sem=send_fa.at[k],
            recv_sem=recv_fa.at[k],
            device_id=(py, px, z, core),
            device_id_type=MESH_ID,
        )

    def feat_copy_z(kz, there, slot):
        return pltpu.make_async_remote_copy(
            src_ref=feats_b.at[me_b],
            dst_ref=feats_b.at[slot],
            send_sem=send_fb.at[kz],
            recv_sem=recv_fb.at[kz],
            device_id=(y, x, there, core),
            device_id_type=MESH_ID,
        )

    def hand_over(kz, source_core, target_core):
        slot = feats_b.at[behind(kz) * nc + source_core]
        return pltpu.make_async_remote_copy(
            src_ref=slot,
            dst_ref=slot,
            send_sem=send_pass.at[kz],
            recv_sem=recv_pass.at[kz],
            device_id=(y, x, z, target_core),
            device_id_type=MESH_ID,
        )

    pl.semaphore_wait(barrier, na + nb - 2)
    for kz in near_z[1:]:
        feat_copy_z(kz, ahead(kz), me_b).start()
    hand_over(0, core, other).start()
    rows_a = [(0, 1), (ny - 1, 2)] if ny == 4 else [(ky,) for ky in range(ny)]
    near_a = [[(ky, kx) for ky in group for kx in range(nx)] for group in rows_a]
    for group in near_a:
        for ky, kx in group:
            if (ky, kx) != (0, 0):
                feat_copy_a(ky, kx, me_a).start()
    send_vector(0, start, none)

    fold = -INV_WIDTH * math.log2(math.e)
    ones = jnp.ones((8, BLOCK), jnp.float32)

    def take_columns(group):
        for ky, kx in group:
            if (ky, kx) != (0, 0):
                feat_copy_a(ky, kx, source_a(ky, kx)).wait_recv()

    def span_of(there):
        return pl.ds(pl.multiple_of(there * width, width), width)

    def rows_at(there):
        return feats_b[pl.ds(there * nc, nc)].reshape(width, BLOCK)

    def take_rows(group):
        for kz in group:
            if kz != 0:
                feat_copy_z(kz, behind(kz), behind(kz) * nc + core).wait_recv()
                hand_over(kz, core, other).start()
        for kz in group:
            hand_over(kz, other, other).wait_recv()
            wide = rows_at(behind(kz)).astype(jnp.float32)
            row_norms[:, span_of(behind(kz))] = fold * lax.dot_general(
                ones,
                wide * wide,
                (((1,), (1,)), ((), ())),
                precision=lax.Precision.HIGHEST,
                preferred_element_type=jnp.float32,
            )

    def fill(columns, rows):
        first_row = columns[0][0]
        row_step = columns[-1][0] - first_row

        @pl.loop(0, len(columns))
        def _(i):
            ai = source_a(first_row + row_step * (i // nx), lax.rem(i, nx))
            cols = feats_a[ai]
            wide = cols.astype(jnp.float32)
            norm = fold * jnp.sum(wide * wide, axis=1, keepdims=True)
            at = pl.ds(pl.multiple_of(ai * BLOCK, BLOCK), BLOCK)
            for kz in rows:
                there = behind(kz)
                span = span_of(there)
                inner = lax.dot_general(
                    cols,
                    rows_at(there),
                    (((1,), (1,)), ((), ())),
                    preferred_element_type=jnp.float32,
                )
                power = jnp.minimum((norm + row_norms[0:1, span]) - (2.0 * fold) * inner, 0.0)
                tile[at, span] = jnp.exp2(power).astype(jnp.bfloat16)

    half = nz // 2
    near_rows, far_rows = near_z[:half], near_z[half:]
    take_columns(near_a[0])
    take_rows(near_rows)
    fill(near_a[0], near_rows)
    take_columns(near_a[1])
    fill(near_a[1], near_rows)
    take_rows(far_rows)
    fill(near_a[0], far_rows)
    fill(near_a[1], far_rows)

    def scalars(total, guess):
        alpha, ss, sq, qq, sw = from_row(total, 5)
        shift = alpha - guess
        square = ss - 2.0 * shift * sq + shift * shift * qq
        return alpha, shift, jnp.sqrt(jnp.maximum(square, 0.0) + FLOOR_BETA), ss, sw

    def step(j, carry):
        sent, last_q, last_w, guess = carry
        par = lax.rem(j, 2)
        sums = take_vectors(par)
        split_vectors(par)
        for kz in offsets_z:
            there = ahead(kz)
            block = product(there)
            for c in range(nc):
                part[there * nc + c, 0:probe_count] = block[:, c * BLOCK : (c + 1) * BLOCK]
                part[there * nc + c, probe_count:MESSAGE] = sums
            for target in partners(there, kz):
                copy_b(kz, target, par, me_b, core).start()
        arrived[par, me_b] = part[me_b]
        take_parts(par)
        received = jnp.sum(arrived[par], axis=0)
        image = received[0:probe_count] + NOISE_LEVEL * sent
        alpha, shift, beta, _, _ = scalars(received[probe_count:MESSAGE], guess)
        first = j == 0
        alpha = jnp.where(first, FIRST_GUESS, alpha)
        shift = jnp.where(first, 0.0, shift)
        beta = jnp.where(first, 1.0, beta)
        q = (sent - shift * last_q) / beta
        w = (image - shift * last_w) / beta
        new = w - alpha * q - beta * last_q
        sums = to_row([total_of(q, w), total_of(new, new), total_of(new, q), total_of(q, q), total_of(new, w)])
        sent_vector(par)
        send_vector(1 - par, new, sums)
        sent_parts(par)
        out[j, 0:probe_count] = q
        before = lax.rem(j + ITERS - 1, ITERS)
        out[before, probe_count : probe_count + 1] = to_row([alpha])
        out[before, probe_count + 1 : probe_count + 2] = to_row([beta])
        return new, q, w, alpha

    column = jnp.zeros((probe_count, 1), jnp.float32)
    last = ITERS - 1
    sent, last_q, _, guess = lax.fori_loop(0, last, step, (start, zeros, zeros, column))
    par = last % 2
    line[me_b] = sent
    for kz in offsets_z:
        for target in partners(ahead(kz), kz):
            copy_line(kz, target, me_b, core).start()
    sums = take_vectors(par)
    split_vectors(par)
    for kz in offsets_z:
        for sz, sc in partners(behind(kz), kz):
            copy_line(kz, (sz, sc), sz * nc + sc, sc).wait_recv()
    products = zeros
    for zi in range(nz):
        block = product(zi)
        for c in range(nc):
            products = products + block[:, c * BLOCK : (c + 1) * BLOCK] * line[zi * nc + c]
    row = sums + to_row([jnp.sum(products, axis=1, keepdims=True)], 5)
    for bi in range(nb):
        part[bi, probe_count:MESSAGE] = row
    for kz in offsets_z:
        for target in partners(ahead(kz), kz):
            copy_b(kz, target, par, me_b, core, sums_row).start()
    arrived[par, me_b, probe_count:MESSAGE] = row
    take_parts(par, sums_row)
    total = jnp.sum(arrived[par, :, probe_count:MESSAGE], axis=0)
    sent_vector(par)
    free = 1 - par
    gathered[free, me_a, probe_count:MESSAGE] = total
    for ky, kx in offsets_a:
        copy_a(ky, kx, free, me_a, sums_row).start()
    alpha, shift, beta, ss, sw = scalars(total, guess)
    out[last, 0:probe_count] = (sent - shift * last_q) / beta
    out[last - 1, probe_count : probe_count + 1] = to_row([alpha])
    out[last - 1, probe_count + 1 : probe_count + 2] = to_row([beta])
    for ky, kx in offsets_a:
        copy_a(ky, kx, free, source_a(ky, kx), sums_row).wait_recv()
    form = from_row(jnp.sum(gathered[free, :, probe_count:MESSAGE], axis=0), 6)[5]
    form = form + NOISE_LEVEL * ss - 2.0 * shift * sw + shift * shift * alpha
    out[last, probe_count : probe_count + 1] = to_row([form / (beta * beta)])
    for ky, kx in offsets_a:
        copy_a(ky, kx, free, me_a, sums_row).wait_send()
        feat_copy_a(ky, kx, me_a).wait_send()
    sent_parts(par, sums_row)
    for kz in offsets_z:
        for target in partners(ahead(kz), kz):
            copy_line(kz, target, me_b, core).wait_send()
        hand_over(kz, core, other).wait_send()
        if kz != 0:
            feat_copy_z(kz, ahead(kz), me_b).wait_send()


def rounds_of(order):
    ring = list(range(1, order))
    result = []
    for _ in range(order - 1):
        line = [0] + ring
        pairs = [(line[i], line[order - 1 - i]) for i in range(order // 2)]
        result.append([(min(p), max(p)) for p in pairs])
        ring = ring[1:] + ring[:1]
    return result


def rotation(first, second, off):
    gap = first - second
    double = 2.0 * off
    scale = jnp.maximum(jnp.abs(gap), jnp.abs(double))
    flat = scale == 0.0
    inverse = 1.0 / jnp.where(flat, 1.0, scale)
    gap = jnp.where(flat, 1.0, gap * inverse)
    double = double * inverse
    norm_inv = lax.rsqrt(gap * gap + double * double)
    cos_two = gap * norm_inv
    sin_two = double * norm_inv
    large = jnp.sqrt(0.5 + 0.5 * jnp.abs(cos_two))
    small = 0.5 * jnp.abs(sin_two) / large
    straight = gap >= 0.0
    cosine = jnp.where(straight, large, small)
    sine = jnp.where(straight, small, large)
    return cosine, jnp.where(double < 0.0, -sine, sine)


def quadrature_kernel(scale_root, lanczos, solves, logdet, scale_grad):
    order, probe_count = lanczos.shape[0], solves.shape[0]
    shape = (order, BLOCK)
    index = lax.broadcasted_iota(jnp.int32, shape, 0)
    diag = [jnp.broadcast_to(lanczos[i, probe_count : probe_count + 1], shape) for i in range(order)]
    off = {}
    for i in range(order):
        for j in range(i + 1, order):
            near = j == i + 1
            band = lanczos[i, probe_count + 1 : probe_count + 2] if near else 0.0
            off[i, j] = jnp.broadcast_to(band, shape)
    vectors = [jnp.where(index == i, 1.0, 0.0).astype(jnp.float32) for i in range(order)]
    keys = sorted(off)

    def sweep(_, state):
        diag, entries, vectors = list(state[0]), dict(zip(keys, state[1])), list(state[2])

        def key(i, j):
            return (i, j) if i < j else (j, i)

        for pairs in rounds_of(order):
            turns = [rotation(diag[p], diag[q], entries[p, q]) for p, q in pairs]
            for (p, q), (c, s) in zip(pairs, turns):
                for k in range(order):
                    if k != p and k != q:
                        one, two = entries[key(p, k)], entries[key(q, k)]
                        entries[key(p, k)] = c * one + s * two
                        entries[key(q, k)] = c * two - s * one
                one, two, cross = diag[p], diag[q], entries[p, q]
                both = 2.0 * c * s * cross
                diag[p] = c * c * one + both + s * s * two
                diag[q] = s * s * one - both + c * c * two
                entries[p, q] = c * s * (two - one) + (c * c - s * s) * cross
                one, two = vectors[p], vectors[q]
                vectors[p] = c * one + s * two
                vectors[q] = c * two - s * one
        return tuple(diag), tuple(entries[k] for k in keys), tuple(vectors)

    state = (tuple(diag), tuple(off[k] for k in keys), tuple(vectors))
    diag, _, vectors = lax.fori_loop(0, SWEEPS, sweep, state)
    log_sum = jnp.zeros(shape, jnp.float32)
    coef = jnp.zeros(shape, jnp.float32)
    for k in range(order):
        value = jnp.maximum(diag[k], EIGEN_FLOOR)
        leading = jnp.broadcast_to(vectors[k][0:1], shape)
        log_sum = log_sum + leading * leading * jnp.log(value)
        coef = coef + vectors[k] * (leading / value)
    logdet[...] = log_sum[0:1, 0:probe_count]
    scale_grad[...] = (1.0 - NOISE_LEVEL * coef)[0:1, 0:probe_count]
    lane = lax.broadcasted_iota(jnp.int32, (probe_count, BLOCK), 1)
    sub = lax.broadcasted_iota(jnp.int32, (probe_count, BLOCK), 0)
    total = jnp.zeros((probe_count, BLOCK), jnp.float32)
    for j in range(order):
        weight = jnp.sum(jnp.where(lane == sub, coef[j : j + 1], 0.0), axis=1, keepdims=True)
        total = total + weight * lanczos[j, 0:probe_count]
    solves[...] = scale_root * total


def local(dims, embeds, w_hidden, b_hidden, w_out, probes):
    ny, nx, nz, nc = dims
    na, nb = ny * nx, nz * nc
    rows, emb = embeds.shape
    probe_count = probes.shape[0]
    feat = w_out.shape[1]
    vmem = pl.BlockSpec(memory_space=pltpu.VMEM)
    hbm = pl.BlockSpec(memory_space=pltpu.HBM)
    lanczos = pl.pallas_call(
        functools.partial(lanczos_kernel, dims),
        out_shape=jax.ShapeDtypeStruct((ITERS, 24, rows), jnp.float32),
        in_specs=[hbm] * 5,
        out_specs=vmem,
        scratch_shapes=[
            pltpu.VMEM((rows, emb), jnp.bfloat16),
            pltpu.VMEM((emb, emb), jnp.bfloat16),
            pltpu.VMEM((1, emb), jnp.float32),
            pltpu.VMEM((emb, feat), jnp.bfloat16),
            pltpu.VMEM((probe_count, rows), jnp.int32),
            pltpu.VMEM((na, rows, feat), jnp.bfloat16),
            pltpu.VMEM((nb, rows, feat), jnp.bfloat16),
            pltpu.VMEM((8, nb * rows), jnp.float32),
            pltpu.VMEM((na * rows, nb * rows), jnp.bfloat16),
            pltpu.VMEM((2, na, 24, rows), jnp.float32),
            pltpu.VMEM((2 * probe_count, na * rows), jnp.bfloat16),
            pltpu.VMEM((nb, 24, rows), jnp.float32),
            pltpu.VMEM((2, nb, 24, rows), jnp.float32),
            pltpu.VMEM((nb, probe_count, rows), jnp.float32),
            pltpu.SemaphoreType.DMA((5,)),
            pltpu.SemaphoreType.DMA((na,)),
            pltpu.SemaphoreType.DMA((na,)),
            pltpu.SemaphoreType.DMA((nz,)),
            pltpu.SemaphoreType.DMA((nz,)),
            pltpu.SemaphoreType.DMA((nz,)),
            pltpu.SemaphoreType.DMA((nz,)),
            pltpu.SemaphoreType.DMA((na,)),
            pltpu.SemaphoreType.DMA((2, na)),
            pltpu.SemaphoreType.DMA((nb,)),
            pltpu.SemaphoreType.DMA((2, nb)),
            pltpu.SemaphoreType.DMA((nb,)),
            pltpu.SemaphoreType.DMA((nb,)),
        ],
        compiler_params=pltpu.CompilerParams(
            collective_id=0, has_side_effects=True, vmem_limit_bytes=60 * 1024 * 1024
        ),
        name="lanczos",
    )(embeds, w_hidden, b_hidden, w_out, probes)
    scale_root = math.sqrt(na * nb * rows)
    small = jax.ShapeDtypeStruct((1, probe_count), jnp.float32)
    solves, logdet, scale_grad = pl.pallas_call(
        functools.partial(quadrature_kernel, scale_root),
        out_shape=(jax.ShapeDtypeStruct((probe_count, rows), jnp.float32), small, small),
        in_specs=[vmem],
        out_specs=(vmem,) * 3,
        name="quadrature",
    )(lanczos)
    return solves, logdet.reshape(probe_count), scale_grad.reshape(probe_count)


def solution(mesh):
    cores = 2
    ny = mesh.shape["grp"]
    nx = 4
    dims = (ny, nx, mesh.shape["row"] // (nx * cores), cores)
    finer = Mesh(mesh.devices.reshape(dims), GRP_ROW)
    return jax.shard_map(
        functools.partial(local, dims),
        mesh=finer,
        in_specs=(P(GRP_ROW, None), P(), P(), P(), P(None, GRP_ROW)),
        out_specs=(P(None, GRP_ROW), P(), P()),
        check_vma=False,
    )
```
